32 devices in a mesh: gx: 8 (over z, y), gy: 4 (over x, core).
Axes of the slice: x: 2, y: 2, z: 4, core: 2. Of those that a mesh axis runs over, the one named last changes fastest.
Arguments:
- residual_block: float32 [8, 32, 32, 256], P(None, 'gx', 'gy'), may hold values from -70 to 70
- diagonal: float32 [32, 32, 256], P('gx', 'gy'), may hold values from 0.5 to 4
Outputs:
- correction: float32 [8, 32, 32, 256], P(None, 'gx', 'gy')
- new_residual: float32 [8, 32, 32, 256], P(None, 'gx', 'gy')
- estimate: float32 [8], replicated
The draws below stay inside these ranges and needn't reach their ends.
All inputs are finite; a program needn't handle non-finite values.
Results may differ from the reference program's by a relative error of at most 0.008.
Values sent between devices are 32-bit elements; how exact they have to be, the bound alone decides.
A program may use at most 64 MiB of HBM per device.

```python
import math
import jax
import jax.numpy as jnp
import numpy as np
from jax import lax

NRHS = 8
NX = 32
NY = 32
NZ = 256


def draw_residual_block(key, part):
    third = jax.random.fold_in(jax.random.fold_in(key, 17), 2)
    coord_x = jnp.arange(NX, dtype=jnp.float32) / NX
    rising = jnp.exp(math.log(3.0) * coord_x)[None, :, None, None]
    values = jnp.clip(jax.random.normal(third, (NRHS, NX, NY, NZ), jnp.float32), -4.0, 4.0)
    return (values * rising).astype(jnp.float32)


def level_of(own_key, shape, cuts, low, top_value):
    factor_of, own = 1.0, jax.random.fold_in(own_key, 6)
    for position, shards_of in cuts:
        heights = jnp.exp(jax.random.uniform(jax.random.fold_in(own, position), (shards_of,), jnp.float32, low / len(cuts), top_value / len(cuts)))
        factor_of = factor_of * jnp.repeat(heights, shape[position] // shards_of).reshape([-1 if axis == position else 1 for axis in range(len(shape))])
    return factor_of


def setup_inputs(seed: int = 0) -> dict:
    streams_of = jax.random.split(jax.random.key(seed), 3)
    residual_block = draw_residual_block(jax.random.fold_in(streams_of[2], 71), 0)
    diagonal = jnp.clip(jnp.exp(math.log(4.0) - 2.0794415 * jax.random.uniform(streams_of[1], (NX, NY, NZ), jnp.float32) ** level_of(streams_of[1], (NX, NY, NZ), ((0, 8), (1, 4)), -0.2, 0.2)), 0.5, 4.0)
    return {"residual_block": residual_block, "diagonal": diagonal}


WEIGHT_X = 0.4
WEIGHT_Y = 0.2
WEIGHT_Z = 0.1
CENTRE = 2.2
SCALE_POWER = 3.0
SHIFTS = (6.0, 1.5, 4.5, 3.0)
EPSILON = 1e-06

def apply_padded(padded, diag_inner, shift_now):
    along_z = jnp.pad(padded, ((0, 0), (0, 0), (0, 0), (1, 1)))
    sum_z = padded + WEIGHT_Z * (along_z[..., :-2] + along_z[..., 2:])
    sum_y = sum_z[:, :, 1:-1] + WEIGHT_Y * (sum_z[:, :, :-2] + sum_z[:, :, 2:])
    sum_x = sum_y[:, 1:-1] + WEIGHT_X * (sum_y[:, :-2] + sum_y[:, 2:])
    centre_cells = padded[:, 1:-1, 1:-1]
    return ((CENTRE + 1.0 + diag_inner - shift_now) * centre_cells - sum_x) / SCALE_POWER

def newton_table():
    blocks = len(SHIFTS)
    identity = np.eye(NRHS, dtype=np.float32)
    matrix = np.zeros(((blocks + 1) * NRHS, blocks * NRHS), np.float32)
    for block_index in range(blocks):
        low = block_index * NRHS
        matrix[low:low + NRHS, low:low + NRHS] = SHIFTS[block_index] * identity
        matrix[low + NRHS:low + 2 * NRHS, low:low + NRHS] = SCALE_POWER * identity
    return matrix

def solve_small(gram_full):
    highest = lax.Precision.HIGHEST
    newton = jnp.asarray(newton_table(), gram_full.dtype)
    image = jnp.dot(newton.T, jnp.dot(gram_full, newton, precision=highest), precision=highest)
    right_side = jnp.dot(newton.T, gram_full[:, :NRHS], precision=highest)
    scales = lax.rsqrt(jnp.diagonal(image) + EPSILON)
    scaled = image * scales[:, None] * scales[None, :]
    factor = jnp.linalg.cholesky(scaled)
    coeffs = scales[:, None] * jax.scipy.linalg.cho_solve((factor, True), scales[:, None] * right_side)
    initial_sq = jnp.diagonal(gram_full)[:NRHS]
    estimate = (initial_sq - lax.optimization_barrier(jnp.sum(right_side * coeffs, axis=0))) / initial_sq
    return (coeffs, jnp.dot(newton, coeffs, precision=highest), estimate)

def reference(residual_block, diagonal):
    highest = lax.Precision.HIGHEST
    powers = [residual_block]
    field_now = residual_block
    for shift_now in SHIFTS:
        padded = jnp.pad(field_now, ((0, 0), (1, 1), (1, 1), (0, 0)))
        field_now = apply_padded(padded, diagonal, shift_now)
        powers.append(field_now)
    basis = jnp.concatenate(powers, 0).reshape(len(powers) * NRHS, -1)
    gram_full = lax.dot_general(basis.astype(jnp.float32), basis.astype(jnp.float32), (((1,), (1,)), ((), ())), precision=highest, preferred_element_type=jnp.float32)
    coeffs, combined, estimate = solve_small(gram_full)
    kept = len(SHIFTS) * NRHS
    correction = lax.dot_general(coeffs.astype(jnp.float32), basis[:kept].astype(jnp.float32), (((0,), (0,)), ((), ())), precision=highest, preferred_element_type=jnp.float32)
    removed = lax.dot_general(combined.astype(jnp.float32), basis.astype(jnp.float32), (((0,), (0,)), ((), ())), precision=highest, preferred_element_type=jnp.float32)
    new_residual = residual_block - removed.reshape(residual_block.shape)
    return (correction.reshape(residual_block.shape), new_residual, estimate)
```

```python
import functools

import jax
import jax.numpy as jnp
from jax import lax
from jax.experimental import pallas as pl
from jax.experimental.pallas import tpu as pltpu
from jax.sharding import PartitionSpec as P

WEIGHT_X = 0.4
WEIGHT_Y = 0.2
WEIGHT_Z = 0.1
CENTRE = 2.2
SCALE_POWER = 3.0
SHIFTS = (6.0, 1.5, 4.5, 3.0)
EPSILON = 1e-06
DEPTH = len(SHIFTS)
MESH = pl.DeviceIdType.MESH
LANES = 128


def kernel(nx, ny, dims, r_ref, d_ref, corr_ref, new_ref, est_ref,
           e_bufs, sy, dd, basis, gram, gather_y, gather_x, wide, halo_send, halo_recv, red_send_y, red_recv_y,
           red_send_x, red_recv_x):
    nf, cx, cy, nz = dims
    dep = DEPTH
    nb = (dep + 1) * nf
    nk = dep * nf
    gx = lax.axis_index("gx")
    gy = lax.axis_index("gy")
    e0 = e_bufs.at[0]
    wx, wy = cx + 2 * dep, cy + 2 * dep
    nt = nz // LANES

    barrier = pltpu.get_barrier_semaphore()
    for k in range(1, nx):
        pl.semaphore_signal(barrier, inc=1, device_id=(lax.rem(gx + k, nx), gy), device_id_type=MESH)
    for k in range(1, ny):
        pl.semaphore_signal(barrier, inc=1, device_id=(gx, lax.rem(gy + k, ny)), device_id_type=MESH)

    for x in range(cx):
        for y in range(cy):
            v = jnp.concatenate([r_ref[pl.ds((x * nt + t) * cy + y, nf, stride=cx * cy * nt), :] for t in range(nt)], 1)
            e0[dep + x, dep + y] = v
            cell = x * cy + y
            basis[0:nf, cell * nz:(cell + 1) * nz] = v
        dd[dep + x, 1] = d_ref[x]

    zero_row = jnp.zeros((dep, cy, nf, nz), jnp.float32)
    zero_col = jnp.zeros((dep, nf, nz), jnp.float32)

    def clear_rows(lo):
        def one(i, c):
            e0[lo + i, dep:dep + cy] = zero_row[0]
            dd[lo + i, 1] = jnp.zeros((cy, nz), jnp.float32)
            return c
        lax.fori_loop(0, dep, one, 0)

    def clear_cols(lo, tile):
        def one(i, c):
            e0[i, lo:lo + dep] = zero_col
            dd[i, tile] = jnp.zeros((cy, nz), jnp.float32)
            return c
        lax.fori_loop(0, wx, one, 0)

    pl.when(gx == 0)(lambda: clear_rows(0))
    pl.when(gx == nx - 1)(lambda: clear_rows(dep + cx))
    pl.when(gy == 0)(lambda: clear_cols(0, 0))
    pl.when(gy == ny - 1)(lambda: clear_cols(dep + cy, 2))

    pl.semaphore_wait(barrier, nx + ny - 2)

    def copy(src, dst, slot, dev):
        return pltpu.make_async_remote_copy(src_ref=src, dst_ref=dst, send_sem=halo_send.at[slot],
                                            recv_sem=halo_recv.at[slot], device_id=dev, device_id_type=MESH)

    own_y = pl.ds(dep, cy)
    up_rows, down_rows = pl.ds(cx, dep), pl.ds(dep, dep)
    up = (gx + 1, gy)
    down = (gx - 1, gy)
    has_up, has_down = gx < nx - 1, gx > 0
    up_copies = [copy(e0.at[up_rows, own_y], e0.at[pl.ds(0, dep), own_y], 0, up),
                 copy(dd.at[up_rows, 1], dd.at[pl.ds(0, dep), 1], 1, up)]
    down_copies = [copy(e0.at[down_rows, own_y], e0.at[pl.ds(dep + cx, dep), own_y], 2, down),
                   copy(dd.at[down_rows, 1], dd.at[pl.ds(dep + cx, dep), 1], 3, down)]

    right, left = (gx, gy + 1), (gx, gy - 1)
    has_right, has_left = gy < ny - 1, gy > 0
    groups = [pl.ds(dep, cx), pl.ds(0, dep), pl.ds(dep + cx, dep)]
    right_copies, left_copies = [], []
    for i, rows in enumerate(groups):
        right_copies.append([copy(e0.at[rows, pl.ds(cy, dep)], e0.at[rows, pl.ds(0, dep)], 4 + 4 * i, right),
                             copy(dd.at[rows, 1], dd.at[rows, 0], 5 + 4 * i, right)])
        left_copies.append([copy(e0.at[rows, pl.ds(dep, dep)], e0.at[rows, pl.ds(dep + cy, dep)], 6 + 4 * i, left),
                            copy(dd.at[rows, 1], dd.at[rows, 2], 7 + 4 * i, left)])

    def start(pred, copies):
        @pl.when(pred)
        def _():
            for c in copies:
                c.start()

    def wait_recv(pred, copies):
        @pl.when(pred)
        def _():
            for c in copies:
                c.wait_recv()

    def wait_send(pred, copies):
        @pl.when(pred)
        def _():
            for c in copies:
                c.wait_send()

    start(has_up, up_copies)
    start(has_down, down_copies)
    start(has_right, right_copies[0])
    start(has_left, left_copies[0])
    wait_recv(has_down, up_copies)
    start(has_right, right_copies[1])
    start(has_left, left_copies[1])
    wait_recv(has_up, down_copies)
    start(has_right, right_copies[2])
    start(has_left, left_copies[2])
    for i in range(3):
        wait_recv(has_left, right_copies[i])
        wait_recv(has_right, left_copies[i])

    lane = lax.broadcasted_iota(jnp.int32, (nf, nz), 1)
    first, last = lane == 0, lane == nz - 1

    def sum_z(v):
        lo = jnp.where(first, 0.0, pltpu.roll(v, 1, 1))
        hi = jnp.where(last, 0.0, pltpu.roll(v, nz - 1, 1))
        return v + WEIGHT_Z * (lo + hi)

    total_x, total_y = cx * nx, cy * ny
    for j, shift in enumerate(SHIFTS):
        src = e_bufs.at[j]
        def row_pass(x, c, src=src, j=j):
            prev = sum_z(src[x, j])
            here = sum_z(src[x, j + 1])
            for y in range(j + 1, wy - j - 1):
                nxt = sum_z(src[x, y + 1])
                sy[x, y] = here + WEIGHT_Y * (prev + nxt)
                prev, here = here, nxt
            return c
        lax.fori_loop(j, wx - j, row_pass, 0)

        def col_pass(x, c, src=src, j=j, shift=shift, keep=False):
            at_x = gx * cx + x - dep
            in_x = (at_x >= 0) & (at_x < total_x)
            for y in range(j + 1, wy - j - 1):
                at_y = gy * cy + y - dep
                factor = jnp.where(in_x & (at_y >= 0) & (at_y < total_y), 1.0 / SCALE_POWER, 0.0)
                tile, sub = (y - dep + cy) // cy, (y - dep) % cy
                diag = dd[x, tile, sub:sub + 1, :]
                centre = src[x, y]
                s = sy[x, y] + WEIGHT_X * (sy[x - 1, y] + sy[x + 1, y])
                v = ((CENTRE + 1.0 - shift + diag) * centre - s) * factor
                if j + 1 < dep:
                    e_bufs[j + 1, x, y] = v
                if keep and dep <= y < dep + cy:
                    cell = (x - dep) * cy + (y - dep)
                    basis[(j + 1) * nf:(j + 2) * nf, pl.ds(pl.multiple_of(cell * nz, nz), nz)] = v
            return c
        if j + 1 < dep:
            lax.fori_loop(j + 1, dep, col_pass, 0)
            lax.fori_loop(dep + cx, wx - j - 1, col_pass, 0)
        lax.fori_loop(dep, dep + cx, functools.partial(col_pass, keep=True), 0)

    b = basis[...]
    local = lax.dot_general(b, b, (((1,), (1,)), ((), ())), precision=lax.Precision.HIGHEST,
                            preferred_element_type=jnp.float32)
    gram[...] = jnp.zeros_like(gram)
    gram[:, 0:nb] = local

    def reduce(buf, value, me, n, send, recv, dev):
        buf[me] = value
        copies = []
        for k in range(1, n):
            to = lax.rem(me + k, n)
            c = pltpu.make_async_remote_copy(src_ref=buf.at[me], dst_ref=buf.at[me], send_sem=send.at[k],
                                             recv_sem=recv.at[k], device_id=dev(to), device_id_type=MESH)
            c.start()
            copies.append(c)
        for k in range(1, n):
            frm = lax.rem(me - k + n, n)
            pltpu.make_async_remote_copy(src_ref=buf.at[frm], dst_ref=buf.at[frm], send_sem=send.at[k],
                                         recv_sem=recv.at[k], device_id=dev(frm), device_id_type=MESH).wait_recv()
        total = buf[0]
        for k in range(1, n):
            total = total + buf[k]
        return total, copies

    part, copies_y = reduce(gather_y, gram[...], gy, ny, red_send_y, red_recv_y, lambda t: (gx, t))
    full, copies_x = reduce(gather_x, part, gx, nx, red_send_x, red_recv_x, lambda t: (t, gy))

    lane_b = lax.broadcasted_iota(jnp.int32, (nb, LANES), 1)
    sigma_lane = jnp.zeros((nb, LANES), jnp.float32)
    for j, shift in enumerate(SHIFTS):
        sigma_lane = jnp.where((lane_b >= j * nf) & (lane_b < (j + 1) * nf), shift, sigma_lane)
    gn = full * sigma_lane + SCALE_POWER * pltpu.roll(full, LANES - nf, 1)

    def newton_rows(m):
        return jnp.concatenate([SHIFTS[j] * m[j * nf:(j + 1) * nf] + SCALE_POWER * m[(j + 1) * nf:(j + 2) * nf]
                                for j in range(dep)], 0)

    image = newton_rows(gn)
    right_side = pltpu.roll(newton_rows(full), nk, 1)
    lane_k = lax.broadcasted_iota(jnp.int32, (nk, LANES), 1)
    row_k = lax.broadcasted_iota(jnp.int32, (nk, LANES), 0)
    on_diag = jnp.where(lane_k == row_k, image, 0.0)
    s_col = lax.rsqrt(jnp.sum(on_diag, axis=1, keepdims=True) + EPSILON)
    s_row = lax.rsqrt(jnp.sum(on_diag, axis=0, keepdims=True) + EPSILON)
    in_image = lane_k < nk
    in_right = (lane_k >= nk) & (lane_k < nk + nf)
    m = jnp.where(in_image, image * s_col * s_row, jnp.where(in_right, right_side * s_col, 0.0))
    for k in range(nk):
        row = m[k:k + 1, :]
        row = row / row[:, k:k + 1]
        m = jnp.where(row_k == k, row, m - m[:, k:k + 1] * row)
    coeffs = jnp.where(in_right, m * s_col, 0.0)

    diag0 = jnp.sum(jnp.where(lane_k[:nf] == row_k[:nf], full[:nf], 0.0), axis=0, keepdims=True)
    used = pltpu.roll(jnp.sum(jnp.where(in_right, right_side * coeffs, 0.0), axis=0, keepdims=True), LANES - nk, 1)
    est_ref[...] = (diag0 - used) / jnp.where(lane_k[:1] < nf, diag0, 1.0)

    blocks = [coeffs[j * nf:(j + 1) * nf] for j in range(dep)]
    combined = [SHIFTS[0] * blocks[0]]
    for j in range(1, dep):
        combined.append(SHIFTS[j] * blocks[j] + SCALE_POWER * blocks[j - 1])
    combined.append(SCALE_POWER * blocks[dep - 1])
    wide[...] = jnp.zeros_like(wide)
    for j in range(dep + 1):
        moved = pltpu.roll(combined[j], nf, 1)
        wide[j * nf:(j + 1) * nf, :] = moved + blocks[j] if j < dep else moved
    weights = jnp.transpose(wide[...])[nk:nk + 2 * nf, 0:nb]
    out = lax.dot_general(weights, basis[...], (((1,), (0,)), ((), ())), precision=lax.Precision.HIGHEST,
                          preferred_element_type=jnp.float32)
    for cell in range(cx * cy):
        x, y = cell // cy, cell % cy
        for t in range(nt):
            span = slice(cell * nz + t * LANES, cell * nz + (t + 1) * LANES)
            rows = pl.ds((x * nt + t) * cy + y, nf, stride=cx * cy * nt)
            corr_ref[rows, :] = out[0:nf, span]
            new_ref[rows, :] = basis[0:nf, span] - out[nf:2 * nf, span]

    wait_send(has_up, up_copies)
    wait_send(has_down, down_copies)
    for i in range(3):
        wait_send(has_right, right_copies[i])
        wait_send(has_left, left_copies[i])
    for c in copies_y + copies_x:
        c.wait_send()


def solution(mesh):
    nx, ny = mesh.shape["gx"], mesh.shape["gy"]

    def body(residual_block, diagonal):
        nf, cx, cy, nz = residual_block.shape
        nb = (DEPTH + 1) * nf
        wx, wy = cx + 2 * DEPTH, cy + 2 * DEPTH
        nt = nz // LANES
        flat = jax.ShapeDtypeStruct((nf * cx * nt * cy, LANES), jnp.float32)

        def tiles(v):
            return v.reshape(nf, cx, cy, nt, LANES).transpose(0, 1, 3, 2, 4).reshape(flat.shape)

        def untile(v):
            return v.reshape(nf, cx, nt, cy, LANES).transpose(0, 1, 3, 2, 4).reshape(nf, cx, cy, nz)

        vmem = pl.BlockSpec(memory_space=pltpu.VMEM)
        corr, new, est = pl.pallas_call(
            functools.partial(kernel, nx, ny, (nf, cx, cy, nz)),
            out_shape=(flat, flat, jax.ShapeDtypeStruct((1, LANES), jnp.float32)),
            in_specs=[vmem, vmem],
            out_specs=(vmem, vmem, vmem),
            scratch_shapes=[
                pltpu.VMEM((DEPTH, wx, wy, nf, nz), jnp.float32),
                pltpu.VMEM((wx, wy, nf, nz), jnp.float32),
                pltpu.VMEM((wx, 3, cy, nz), jnp.float32),
                pltpu.VMEM((nb, cx * cy * nz), jnp.float32),
                pltpu.VMEM((nb, LANES), jnp.float32),
                pltpu.VMEM((ny, nb, LANES), jnp.float32),
                pltpu.VMEM((nx, nb, LANES), jnp.float32),
                pltpu.VMEM((LANES, LANES), jnp.float32),
                pltpu.SemaphoreType.DMA((16,)),
                pltpu.SemaphoreType.DMA((16,)),
                pltpu.SemaphoreType.DMA((ny,)),
                pltpu.SemaphoreType.DMA((ny,)),
                pltpu.SemaphoreType.DMA((nx,)),
                pltpu.SemaphoreType.DMA((nx,)),
            ],
            compiler_params=pltpu.CompilerParams(collective_id=0, has_side_effects=True),
        )(tiles(residual_block), diagonal)
        return untile(corr), untile(new), est[0, :nf]

    return jax.shard_map(body, mesh=mesh, in_specs=(P(None, "gx", "gy", None), P("gx", "gy", None)),
                         out_specs=(P(None, "gx", "gy", None), P(None, "gx", "gy", None), P()), check_vma=False)
```

```python
import functools

import jax
import jax.numpy as jnp
from jax import lax
from jax.experimental import pallas as pl
from jax.experimental.pallas import tpu as pltpu
from jax.sharding import PartitionSpec as P

WEIGHT_X = 0.4
WEIGHT_Y = 0.2
WEIGHT_Z = 0.1
CENTRE = 2.2
SCALE_POWER = 3.0
SHIFTS = (6.0, 1.5, 4.5, 3.0)
EPSILON = 1e-06
DEPTH = len(SHIFTS)
MESH = pl.DeviceIdType.MESH
LANES = 128


def kernel(nx, ny, dims, r_ref, d_ref, corr_ref, new_ref, est_ref,
           e_bufs, sy, dd, basis, gram, gather_y, gather_x, wide, halo_send, halo_recv, red_send_y, red_recv_y,
           red_send_x, red_recv_x):
    nf, cx, cy, nz = dims
    dep = DEPTH
    nb = (dep + 1) * nf
    nk = dep * nf
    gx = lax.axis_index("gx")
    gy = lax.axis_index("gy")
    e0 = e_bufs.at[0]
    wx, wy = cx + 2 * dep, cy + 2 * dep
    nt = nz // LANES

    barrier = pltpu.get_barrier_semaphore()
    for k in range(1, nx):
        pl.semaphore_signal(barrier, inc=1, device_id=(lax.rem(gx + k, nx), gy), device_id_type=MESH)
    for k in range(1, ny):
        pl.semaphore_signal(barrier, inc=1, device_id=(gx, lax.rem(gy + k, ny)), device_id_type=MESH)

    for x in range(cx):
        for y in range(cy):
            v = jnp.concatenate([r_ref[pl.ds((x * nt + t) * cy + y, nf, stride=cx * cy * nt), :] for t in range(nt)], 1)
            e0[dep + x, dep + y] = v
            cell = x * cy + y
            basis[0:nf, cell * nz:(cell + 1) * nz] = v
        dd[dep + x, 1] = d_ref[x]

    even = lax.rem(gx, 2) == 0
    partner = jnp.where(even, gx + 1, gx - 1)
    beyond = jnp.where(even, gx + 2, gx - 2)
    can_forward = (beyond >= 0) & (beyond < nx)
    gets_forward = (gx > 0) & (gx < nx - 1)
    has_right, has_left = gy < ny - 1, gy > 0
    near = jnp.where(even, dep + cx, 0)
    far = jnp.where(even, 0, dep + cx)

    @pl.when(jnp.logical_not(gets_forward))
    def _():
        def one(i, c):
            e0[far + i] = jnp.zeros((wy, nf, nz), jnp.float32)
            dd[far + i] = jnp.zeros((3, cy, nz), jnp.float32)
            return c
        lax.fori_loop(0, dep, one, 0)

    def clear_cols(lo, tile):
        def one(i, c):
            e0[i, lo:lo + dep] = jnp.zeros((dep, nf, nz), jnp.float32)
            dd[i, tile] = jnp.zeros((cy, nz), jnp.float32)
            return c
        lax.fori_loop(0, wx, one, 0)

    pl.when(gy == 0)(lambda: clear_cols(0, 0))
    pl.when(gy == ny - 1)(lambda: clear_cols(dep + cy, 2))

    pl.semaphore_wait(barrier, nx + ny - 2)

    def copy(src, dst, slot, dev):
        return pltpu.make_async_remote_copy(src_ref=src, dst_ref=dst, send_sem=halo_send.at[slot],
                                            recv_sem=halo_recv.at[slot], device_id=dev, device_id_type=MESH)

    own_y = pl.ds(dep, cy)
    step = dep + 1
    swap = [copy(dd.at[pl.ds(dep, cx), 1], dd.at[pl.ds(far, cx), 1], 0, (partner, gy))]
    swap += [copy(e0.at[dep + i, own_y], e0.at[far + i, own_y], 1 + i, (partner, gy)) for i in range(cx)]
    forward = [copy(dd.at[pl.ds(near, cx), 1], dd.at[pl.ds(far, cx), 1], step, (beyond, gy))]
    forward += [copy(e0.at[near + i, own_y], e0.at[far + i, own_y], step + 1 + i, (beyond, gy)) for i in range(cx)]

    def edges(rows, drows, slot, d_only=False):
        right, left = (gx, gy + 1), (gx, gy - 1)
        if d_only:
            return (copy(dd.at[drows, 1], dd.at[drows, 0], slot, right),
                    copy(dd.at[drows, 1], dd.at[drows, 2], slot + 1, left))
        return (copy(e0.at[rows, pl.ds(cy, dep)], e0.at[rows, pl.ds(0, dep)], slot, right),
                copy(e0.at[rows, pl.ds(dep, dep)], e0.at[rows, pl.ds(dep + cy, dep)], slot + 1, left))

    base = 2 * step
    own_edges = [edges(None, pl.ds(dep, cx), base, True), edges(pl.ds(dep, cx), None, base + 2)]
    base += 4
    near_edges = [edges(None, pl.ds(near, cx), base, True)]
    near_edges += [edges(near + i, None, base + 2 + 2 * i) for i in range(cx)]
    base += 2 * step
    far_edges = [edges(None, pl.ds(far, cx), base, True)]
    far_edges += [edges(far + i, None, base + 2 + 2 * i) for i in range(cx)]

    def when(pred, act):
        pl.when(pred)(act)

    def start_edges(pair, pred=True):
        when(has_right & pred, lambda: pair[0].start())
        when(has_left & pred, lambda: pair[1].start())

    def wait_edges(pairs, pred=True):
        def low():
            for pair in pairs:
                pair[0].wait_recv()

        def high():
            for pair in pairs:
                pair[1].wait_recv()
        when(has_left & pred, low)
        when(has_right & pred, high)

    for c in swap:
        c.start()
    for pair in own_edges:
        start_edges(pair)
    for i in range(step):
        swap[i].wait_recv()
        when(can_forward, lambda i=i: forward[i].start())
        start_edges(near_edges[i])

    def take_far(i):
        when(gets_forward, lambda: forward[i].wait_recv())
        start_edges(far_edges[i], gets_forward)

    lane = lax.broadcasted_iota(jnp.int32, (nf, nz), 1)
    first, last = lane == 0, lane == nz - 1

    def sum_z(v):
        lo = jnp.where(first, 0.0, pltpu.roll(v, 1, 1))
        hi = jnp.where(last, 0.0, pltpu.roll(v, nz - 1, 1))
        return v + WEIGHT_Z * (lo + hi)

    total_x, total_y = cx * nx, cy * ny

    def row_pass(j, x):
        src = e_bufs.at[j]
        prev = sum_z(src[x, j])
        here = sum_z(src[x, j + 1])
        for y in range(j + 1, wy - j - 1):
            nxt = sum_z(src[x, y + 1])
            sy[j, x, y] = here + WEIGHT_Y * (prev + nxt)
            prev, here = here, nxt

    def col_pass(j, x):
        at_x = gx * cx + x - dep
        in_x = (at_x >= 0) & (at_x < total_x)
        for y in range(j + 1, wy - j - 1):
            at_y = gy * cy + y - dep
            factor = jnp.where(in_x & (at_y >= 0) & (at_y < total_y), 1.0 / SCALE_POWER, 0.0)
            tile, sub = (y - dep + cy) // cy, (y - dep) % cy
            diag = dd[x, tile, sub:sub + 1, :]
            s = sy[j, x, y] + WEIGHT_X * (sy[j, x - 1, y] + sy[j, x + 1, y])
            v = ((CENTRE + 1.0 - SHIFTS[j] + diag) * e_bufs[j, x, y] - s) * factor
            if j + 1 < dep:
                e_bufs[j + 1, x, y] = v
            else:
                cell = (x - dep) * cy + (y - dep)
                basis[dep * nf:(dep + 1) * nf, pl.ds(pl.multiple_of(cell * nz, nz), nz)] = v

    def sweep(one, j, lo, count):
        def body(i, c):
            one(j, lo + i)
            return c
        if count > 0:
            lax.fori_loop(0, count, body, 0)

    wait_edges(own_edges)
    wait_edges(near_edges)
    take_far(0)
    for j in range(dep):
        lo = jnp.where(even, dep + j, j)
        sweep(row_pass, j, lo, cx + dep - 2 * j)
        sweep(col_pass, j, lo + 1, cx + dep - 2 - 2 * j)
        take_far(1 + j)
    wait_edges(far_edges, gets_forward)
    for j in range(dep):
        sweep(row_pass, j, jnp.where(even, j, cx + dep - j), dep)
        sweep(col_pass, j, jnp.where(even, j + 1, cx + dep - 1 - j), dep)
    for j in range(1, dep):
        for cell in range(cx * cy):
            basis[j * nf:(j + 1) * nf, cell * nz:(cell + 1) * nz] = e_bufs[j, dep + cell // cy, dep + cell % cy]

    b = basis[...]
    local = lax.dot_general(b, b, (((1,), (1,)), ((), ())), precision=lax.Precision.HIGHEST,
                            preferred_element_type=jnp.float32)
    gram[...] = jnp.zeros_like(gram)
    gram[:, 0:nb] = local

    def reduce(buf, value, me, n, send, recv, dev):
        buf[me] = value
        copies = []
        for k in range(1, n):
            to = lax.rem(me + k, n)
            c = pltpu.make_async_remote_copy(src_ref=buf.at[me], dst_ref=buf.at[me], send_sem=send.at[k],
                                             recv_sem=recv.at[k], device_id=dev(to), device_id_type=MESH)
            c.start()
            copies.append(c)
        for k in range(1, n):
            frm = lax.rem(me - k + n, n)
            pltpu.make_async_remote_copy(src_ref=buf.at[frm], dst_ref=buf.at[frm], send_sem=send.at[k],
                                         recv_sem=recv.at[k], device_id=dev(frm), device_id_type=MESH).wait_recv()
        total = buf[0]
        for k in range(1, n):
            total = total + buf[k]
        return total, copies

    lane_f = lax.broadcasted_iota(jnp.int32, (nf, LANES), 1)

    def turn(v, by):
        return pltpu.roll(v, by % LANES, 1) if by % LANES else v

    packed = jnp.zeros((nf, LANES), jnp.float32)
    for j in range(dep + 1):
        kept = jnp.where(lane_f < (j + 1) * nf, gram[j * nf:(j + 1) * nf, :], 0.0)
        packed = packed + turn(kept, nf * j * (j + 1) // 2)
    part, copies_y = reduce(gather_y, packed, gy, ny, red_send_y, red_recv_y, lambda t: (gx, t))
    whole, copies_x = reduce(gather_x, part, gx, nx, red_send_x, red_recv_x, lambda t: (t, gy))
    wide[...] = jnp.zeros_like(wide)
    for j in range(dep + 1):
        wide[j * nf:(j + 1) * nf, :] = jnp.where(lane_f < (j + 1) * nf, turn(whole, -(nf * j * (j + 1) // 2)), 0.0)
    lower = wide[...]
    upper = jnp.transpose(lower)[0:nb]
    lower = lower[0:nb]
    block_row = lax.broadcasted_iota(jnp.int32, (nb, LANES), 0) // nf
    full = jnp.where(lax.broadcasted_iota(jnp.int32, (nb, LANES), 1) < (block_row + 1) * nf, lower, upper)

    lane_b = lax.broadcasted_iota(jnp.int32, (nb, LANES), 1)
    sigma_lane = jnp.zeros((nb, LANES), jnp.float32)
    for j, shift in enumerate(SHIFTS):
        sigma_lane = jnp.where((lane_b >= j * nf) & (lane_b < (j + 1) * nf), shift, sigma_lane)
    gn = full * sigma_lane + SCALE_POWER * pltpu.roll(full, LANES - nf, 1)

    def newton_rows(m):
        return jnp.concatenate([SHIFTS[j] * m[j * nf:(j + 1) * nf] + SCALE_POWER * m[(j + 1) * nf:(j + 2) * nf]
                                for j in range(dep)], 0)

    image = newton_rows(gn)
    right_side = pltpu.roll(newton_rows(full), nk, 1)
    lane_k = lax.broadcasted_iota(jnp.int32, (nk, LANES), 1)
    row_k = lax.broadcasted_iota(jnp.int32, (nk, LANES), 0)
    on_diag = jnp.where(lane_k == row_k, image, 0.0)
    s_col = lax.rsqrt(jnp.sum(on_diag, axis=1, keepdims=True) + EPSILON)
    s_row = lax.rsqrt(jnp.sum(on_diag, axis=0, keepdims=True) + EPSILON)
    in_image = lane_k < nk
    in_right = (lane_k >= nk) & (lane_k < nk + nf)
    m = jnp.where(in_image, image * s_col * s_row, jnp.where(in_right, right_side * s_col, 0.0))
    for k in range(nk):
        row = m[k:k + 1, :]
        row = row / row[:, k:k + 1]
        m = jnp.where(row_k == k, row, m - m[:, k:k + 1] * row)
    coeffs = jnp.where(in_right, m * s_col, 0.0)

    diag0 = jnp.sum(jnp.where(lane_k[:nf] == row_k[:nf], full[:nf], 0.0), axis=0, keepdims=True)
    used = pltpu.roll(jnp.sum(jnp.where(in_right, right_side * coeffs, 0.0), axis=0, keepdims=True), LANES - nk, 1)
    est_ref[...] = (diag0 - used) / jnp.where(lane_k[:1] < nf, diag0, 1.0)

    blocks = [coeffs[j * nf:(j + 1) * nf] for j in range(dep)]
    combined = [SHIFTS[0] * blocks[0]]
    for j in range(1, dep):
        combined.append(SHIFTS[j] * blocks[j] + SCALE_POWER * blocks[j - 1])
    combined.append(SCALE_POWER * blocks[dep - 1])
    wide[...] = jnp.zeros_like(wide)
    for j in range(dep + 1):
        moved = pltpu.roll(combined[j], nf, 1)
        wide[j * nf:(j + 1) * nf, :] = moved + blocks[j] if j < dep else moved
    weights = jnp.transpose(wide[...])[nk:nk + 2 * nf, 0:nb]
    out = lax.dot_general(weights, basis[...], (((1,), (0,)), ((), ())), precision=lax.Precision.HIGHEST,
                          preferred_element_type=jnp.float32)
    for cell in range(cx * cy):
        x, y = cell // cy, cell % cy
        for t in range(nt):
            span = slice(cell * nz + t * LANES, cell * nz + (t + 1) * LANES)
            rows = pl.ds((x * nt + t) * cy + y, nf, stride=cx * cy * nt)
            corr_ref[rows, :] = out[0:nf, span]
            new_ref[rows, :] = basis[0:nf, span] - out[nf:2 * nf, span]

    for i in range(step):
        swap[i].wait_send()
        when(can_forward, lambda i=i: forward[i].wait_send())
    for pairs, pred in ((own_edges, True), (near_edges, True), (far_edges, gets_forward)):
        for pair in pairs:
            when(has_right & pred, lambda pair=pair: pair[0].wait_send())
            when(has_left & pred, lambda pair=pair: pair[1].wait_send())
    for c in copies_y + copies_x:
        c.wait_send()


def solution(mesh):
    nx, ny = mesh.shape["gx"], mesh.shape["gy"]

    def body(residual_block, diagonal):
        nf, cx, cy, nz = residual_block.shape
        nb = (DEPTH + 1) * nf
        wx, wy = cx + 2 * DEPTH, cy + 2 * DEPTH
        nt = nz // LANES
        flat = jax.ShapeDtypeStruct((nf * cx * nt * cy, LANES), jnp.float32)

        def tiles(v):
            return v.reshape(nf, cx, cy, nt, LANES).transpose(0, 1, 3, 2, 4).reshape(flat.shape)

        def untile(v):
            return v.reshape(nf, cx, nt, cy, LANES).transpose(0, 1, 3, 2, 4).reshape(nf, cx, cy, nz)

        assert cx == DEPTH and nx % 2 == 0
        halo_slots = 2 * (DEPTH + 1) + 4 + 4 * (DEPTH + 1)
        vmem = pl.BlockSpec(memory_space=pltpu.VMEM)
        corr, new, est = pl.pallas_call(
            functools.partial(kernel, nx, ny, (nf, cx, cy, nz)),
            out_shape=(flat, flat, jax.ShapeDtypeStruct((1, LANES), jnp.float32)),
            in_specs=[vmem, vmem],
            out_specs=(vmem, vmem, vmem),
            scratch_shapes=[
                pltpu.VMEM((DEPTH, wx, wy, nf, nz), jnp.float32),
                pltpu.VMEM((DEPTH, wx, wy, nf, nz), jnp.float32),
                pltpu.VMEM((wx, 3, cy, nz), jnp.float32),
                pltpu.VMEM((nb, cx * cy * nz), jnp.float32),
                pltpu.VMEM((nb, LANES), jnp.float32),
                pltpu.VMEM((ny, nf, LANES), jnp.float32),
                pltpu.VMEM((nx, nf, LANES), jnp.float32),
                pltpu.VMEM((LANES, LANES), jnp.float32),
                pltpu.SemaphoreType.DMA((halo_slots,)),
                pltpu.SemaphoreType.DMA((halo_slots,)),
                pltpu.SemaphoreType.DMA((ny,)),
                pltpu.SemaphoreType.DMA((ny,)),
                pltpu.SemaphoreType.DMA((nx,)),
                pltpu.SemaphoreType.DMA((nx,)),
            ],
            compiler_params=pltpu.CompilerParams(collective_id=0, has_side_effects=True, vmem_limit_bytes=24 << 20),
        )(tiles(residual_block), diagonal)
        return untile(corr), untile(new), est[0, :nf]

    return jax.shard_map(body, mesh=mesh, in_specs=(P(None, "gx", "gy", None), P("gx", "gy", None)),
                         out_specs=(P(None, "gx", "gy", None), P(None, "gx", "gy", None), P()), check_vma=False)
```

```python
import functools

import jax
import jax.numpy as jnp
from jax import lax
from jax.experimental import pallas as pl
from jax.experimental.pallas import tpu as pltpu
from jax.sharding import PartitionSpec as P

WEIGHT_X = 0.4
WEIGHT_Y = 0.2
WEIGHT_Z = 0.1
CENTRE = 2.2
SCALE_POWER = 3.0
SHIFTS = (6.0, 1.5, 4.5, 3.0)
EPSILON = 1e-06
DEPTH = len(SHIFTS)
MESH = pl.DeviceIdType.MESH
LANES = 128


def kernel(nx, ny, dims, r_hbm, d_hbm, basis, small_ref, r_ref, d_ref, load_sem,
           e_bufs, sy, dd, gram, gather_y, gather_x, wide, halo_send, halo_recv, red_send_y, red_recv_y,
           red_send_x, red_recv_x):
    nf, cx, cy, nz = dims
    dep = DEPTH
    nb = (dep + 1) * nf
    nk = dep * nf
    gx = lax.axis_index("gx")
    gy = lax.axis_index("gy")
    e0 = e_bufs.at[0]
    wx, wy = cx + 2 * dep, cy + 2 * dep
    nt = nz // LANES

    barrier = pltpu.get_barrier_semaphore()
    for k in range(1, nx):
        pl.semaphore_signal(barrier, inc=1, device_id=(lax.rem(gx + k, nx), gy), device_id_type=MESH)
    for k in range(1, ny):
        pl.semaphore_signal(barrier, inc=1, device_id=(gx, lax.rem(gy + k, ny)), device_id_type=MESH)

    loads = [pltpu.make_async_copy(r_hbm, r_ref, load_sem.at[0]), pltpu.make_async_copy(d_hbm, d_ref, load_sem.at[1])]
    for c in loads:
        c.start()
    even = lax.rem(gx, 2) == 0
    partner = jnp.where(even, gx + 1, gx - 1)
    beyond = jnp.where(even, gx + 2, gx - 2)
    can_forward = (beyond >= 0) & (beyond < nx)
    gets_forward = (gx > 0) & (gx < nx - 1)
    has_right, has_left = gy < ny - 1, gy > 0
    near = jnp.where(even, dep + cx, 0)
    far = jnp.where(even, 0, dep + cx)

    @pl.when(jnp.logical_not(gets_forward))
    def _():
        def one(i, c):
            e0[far + i] = jnp.zeros((wy, nf, nz), jnp.float32)
            dd[far + i] = jnp.zeros((3, cy, nz), jnp.float32)
            return c
        lax.fori_loop(0, dep, one, 0)

    def clear_cols(lo, tile):
        def one(i, c):
            e0[i, lo:lo + dep] = jnp.zeros((dep, nf, nz), jnp.float32)
            dd[i, tile] = jnp.zeros((cy, nz), jnp.float32)
            return c
        lax.fori_loop(0, wx, one, 0)

    pl.when(gy == 0)(lambda: clear_cols(0, 0))
    pl.when(gy == ny - 1)(lambda: clear_cols(dep + cy, 2))

    for c in loads:
        c.wait()

    for x in range(cx):
        for y in range(cy):
            v = jnp.concatenate([r_ref[pl.ds((x * nt + t) * cy + y, nf, stride=cx * cy * nt), :] for t in range(nt)], 1)
            e0[dep + x, dep + y] = v
            cell = x * cy + y
            basis[0:nf, cell * nz:(cell + 1) * nz] = v
        dd[dep + x, 1] = d_ref[x]

    pl.semaphore_wait(barrier, nx + ny - 2)

    def copy(src, dst, slot, dev):
        return pltpu.make_async_remote_copy(src_ref=src, dst_ref=dst, send_sem=halo_send.at[slot],
                                            recv_sem=halo_recv.at[slot], device_id=dev, device_id_type=MESH)

    own_y = pl.ds(dep, cy)
    step = dep + 1
    swap = [copy(dd.at[pl.ds(dep, cx), 1], dd.at[pl.ds(far, cx), 1], 0, (partner, gy))]
    swap += [copy(e0.at[dep + i, own_y], e0.at[far + i, own_y], 1 + i, (partner, gy)) for i in range(cx)]
    forward = [copy(dd.at[pl.ds(near, cx), 1], dd.at[pl.ds(far, cx), 1], step, (beyond, gy))]
    forward += [copy(e0.at[near + i, own_y], e0.at[far + i, own_y], step + 1 + i, (beyond, gy)) for i in range(cx)]

    def edges(rows, drows, slot, d_only=False):
        right, left = (gx, gy + 1), (gx, gy - 1)
        if d_only:
            return (copy(dd.at[drows, 1], dd.at[drows, 0], slot, right),
                    copy(dd.at[drows, 1], dd.at[drows, 2], slot + 1, left))
        return (copy(e0.at[rows, pl.ds(cy, dep)], e0.at[rows, pl.ds(0, dep)], slot, right),
                copy(e0.at[rows, pl.ds(dep, dep)], e0.at[rows, pl.ds(dep + cy, dep)], slot + 1, left))

    base = 2 * step
    own_edges = [edges(None, pl.ds(dep, cx), base, True), edges(pl.ds(dep, cx), None, base + 2)]
    base += 4
    near_edges = [edges(None, pl.ds(near, cx), base, True)]
    near_edges += [edges(near + i, None, base + 2 + 2 * i) for i in range(cx)]
    base += 2 * step
    far_edges = [edges(None, pl.ds(far, cx), base, True)]
    far_edges += [edges(far + i, None, base + 2 + 2 * i) for i in range(cx)]

    def when(pred, act):
        pl.when(pred)(act)

    def start_edges(pair, pred=True):
        when(has_right & pred, lambda: pair[0].start())
        when(has_left & pred, lambda: pair[1].start())

    def wait_edges(pairs, pred=True):
        def low():
            for pair in pairs:
                pair[0].wait_recv()

        def high():
            for pair in pairs:
                pair[1].wait_recv()
        when(has_left & pred, low)
        when(has_right & pred, high)

    for c in swap:
        c.start()
    for pair in own_edges:
        start_edges(pair)
    for i in range(step):
        swap[i].wait_recv()
        when(can_forward, lambda i=i: forward[i].start())
        start_edges(near_edges[i])

    def take_far(i):
        when(gets_forward, lambda: forward[i].wait_recv())
        start_edges(far_edges[i], gets_forward)

    lane = lax.broadcasted_iota(jnp.int32, (nf, nz), 1)
    first, last = lane == 0, lane == nz - 1

    def sum_z(v):
        lo = jnp.where(first, 0.0, pltpu.roll(v, 1, 1))
        hi = jnp.where(last, 0.0, pltpu.roll(v, nz - 1, 1))
        return v + WEIGHT_Z * (lo + hi)

    total_x, total_y = cx * nx, cy * ny

    def row_pass(j, x):
        src = e_bufs.at[j]
        prev = sum_z(src[x, j])
        here = sum_z(src[x, j + 1])
        for y in range(j + 1, wy - j - 1):
            nxt = sum_z(src[x, y + 1])
            sy[j, x, y] = here + WEIGHT_Y * (prev + nxt)
            prev, here = here, nxt

    def col_pass(j, x):
        at_x = gx * cx + x - dep
        in_x = (at_x >= 0) & (at_x < total_x)
        for y in range(j + 1, wy - j - 1):
            at_y = gy * cy + y - dep
            factor = jnp.where(in_x & (at_y >= 0) & (at_y < total_y), 1.0 / SCALE_POWER, 0.0)
            tile, sub = (y - dep + cy) // cy, (y - dep) % cy
            diag = dd[x, tile, sub:sub + 1, :]
            s = sy[j, x, y] + WEIGHT_X * (sy[j, x - 1, y] + sy[j, x + 1, y])
            v = ((CENTRE + 1.0 - SHIFTS[j] + diag) * e_bufs[j, x, y] - s) * factor
            if j + 1 < dep:
                e_bufs[j + 1, x, y] = v
            else:
                cell = (x - dep) * cy + (y - dep)
                basis[dep * nf:(dep + 1) * nf, pl.ds(pl.multiple_of(cell * nz, nz), nz)] = v

    def sweep(one, j, lo, count):
        def body(i, c):
            one(j, lo + i)
            return c
        if count > 0:
            lax.fori_loop(0, count, body, 0)

    wait_edges(own_edges)
    wait_edges(near_edges)
    take_far(0)
    for j in range(dep):
        lo = jnp.where(even, dep + j, j)
        sweep(row_pass, j, lo, cx + dep - 2 * j)
        sweep(col_pass, j, lo + 1, cx + dep - 2 - 2 * j)
        take_far(1 + j)
    wait_edges(far_edges, gets_forward)
    for j in range(dep):
        sweep(row_pass, j, jnp.where(even, j, cx + dep - j), dep)
        sweep(col_pass, j, jnp.where(even, j + 1, cx + dep - 1 - j), dep)
    for j in range(1, dep):
        for cell in range(cx * cy):
            basis[j * nf:(j + 1) * nf, cell * nz:(cell + 1) * nz] = e_bufs[j, dep + cell // cy, dep + cell % cy]

    b = basis[...]
    local = lax.dot_general(b, b, (((1,), (1,)), ((), ())), precision=lax.Precision.HIGHEST,
                            preferred_element_type=jnp.float32)
    gram[...] = jnp.zeros_like(gram)
    gram[:, 0:nb] = local

    def reduce(buf, value, me, n, send, recv, dev):
        buf[me] = value
        copies = []
        for k in range(1, n):
            to = lax.rem(me + k, n)
            c = pltpu.make_async_remote_copy(src_ref=buf.at[me], dst_ref=buf.at[me], send_sem=send.at[k],
                                             recv_sem=recv.at[k], device_id=dev(to), device_id_type=MESH)
            c.start()
            copies.append(c)
        for k in range(1, n):
            frm = lax.rem(me - k + n, n)
            pltpu.make_async_remote_copy(src_ref=buf.at[frm], dst_ref=buf.at[frm], send_sem=send.at[k],
                                         recv_sem=recv.at[k], device_id=dev(frm), device_id_type=MESH).wait_recv()
        total = buf[0]
        for k in range(1, n):
            total = total + buf[k]
        return total, copies

    lane_f = lax.broadcasted_iota(jnp.int32, (nf, LANES), 1)

    def turn(v, by):
        return pltpu.roll(v, by % LANES, 1) if by % LANES else v

    packed = jnp.zeros((nf, LANES), jnp.float32)
    for j in range(dep + 1):
        kept = jnp.where(lane_f < (j + 1) * nf, gram[j * nf:(j + 1) * nf, :], 0.0)
        packed = packed + turn(kept, nf * j * (j + 1) // 2)
    part, copies_y = reduce(gather_y, packed, gy, ny, red_send_y, red_recv_y, lambda t: (gx, t))
    whole, copies_x = reduce(gather_x, part, gx, nx, red_send_x, red_recv_x, lambda t: (t, gy))
    wide[...] = jnp.zeros_like(wide)
    for j in range(dep + 1):
        wide[j * nf:(j + 1) * nf, :] = jnp.where(lane_f < (j + 1) * nf, turn(whole, -(nf * j * (j + 1) // 2)), 0.0)
    lower = wide[...]
    upper = jnp.transpose(lower)[0:nb]
    lower = lower[0:nb]
    block_row = lax.broadcasted_iota(jnp.int32, (nb, LANES), 0) // nf
    full = jnp.where(lax.broadcasted_iota(jnp.int32, (nb, LANES), 1) < (block_row + 1) * nf, lower, upper)

    lane_b = lax.broadcasted_iota(jnp.int32, (nb, LANES), 1)
    sigma_lane = jnp.zeros((nb, LANES), jnp.float32)
    for j, shift in enumerate(SHIFTS):
        sigma_lane = jnp.where((lane_b >= j * nf) & (lane_b < (j + 1) * nf), shift, sigma_lane)
    gn = full * sigma_lane + SCALE_POWER * pltpu.roll(full, LANES - nf, 1)

    def newton_rows(m):
        return jnp.concatenate([SHIFTS[j] * m[j * nf:(j + 1) * nf] + SCALE_POWER * m[(j + 1) * nf:(j + 2) * nf]
                                for j in range(dep)], 0)

    image = newton_rows(gn)
    right_side = pltpu.roll(newton_rows(full), nk, 1)
    lane_k = lax.broadcasted_iota(jnp.int32, (nk, LANES), 1)
    row_k = lax.broadcasted_iota(jnp.int32, (nk, LANES), 0)
    on_diag = jnp.where(lane_k == row_k, image, 0.0)
    s_col = lax.rsqrt(jnp.sum(on_diag, axis=1, keepdims=True) + EPSILON)
    s_row = lax.rsqrt(jnp.sum(on_diag, axis=0, keepdims=True) + EPSILON)
    in_image = lane_k < nk
    in_right = (lane_k >= nk) & (lane_k < nk + nf)
    m = jnp.where(in_image, image * s_col * s_row, jnp.where(in_right, right_side * s_col, 0.0))
    for k in range(nk):
        row = m[k:k + 1, :]
        row = row / row[:, k:k + 1]
        m = jnp.where(row_k == k, row, m - m[:, k:k + 1] * row)
    coeffs = jnp.where(in_right, m * s_col, 0.0)

    diag0 = jnp.sum(jnp.where(lane_k[:nf] == row_k[:nf], full[:nf], 0.0), axis=0, keepdims=True)
    used = pltpu.roll(jnp.sum(jnp.where(in_right, right_side * coeffs, 0.0), axis=0, keepdims=True), LANES - nk, 1)
    blocks = [coeffs[j * nf:(j + 1) * nf] for j in range(dep)]
    combined = [SHIFTS[0] * blocks[0]]
    for j in range(1, dep):
        combined.append(SHIFTS[j] * blocks[j] + SCALE_POWER * blocks[j - 1])
    combined.append(SCALE_POWER * blocks[dep - 1])
    wide[...] = jnp.zeros_like(wide)
    for j in range(dep + 1):
        moved = pltpu.roll(combined[j], nf, 1)
        wide[j * nf:(j + 1) * nf, :] = moved + blocks[j] if j < dep else moved
    small_ref[0:2 * nf, :] = jnp.transpose(wide[...])[nk:nk + 2 * nf, :]
    small_ref[2 * nf:, :] = jnp.broadcast_to((diag0 - used) / jnp.where(lane_k[:1] < nf, diag0, 1.0), (nf, LANES))

    for i in range(step):
        swap[i].wait_send()
        when(can_forward, lambda i=i: forward[i].wait_send())
    for pairs, pred in ((own_edges, True), (near_edges, True), (far_edges, gets_forward)):
        for pair in pairs:
            when(has_right & pred, lambda pair=pair: pair[0].wait_send())
            when(has_left & pred, lambda pair=pair: pair[1].wait_send())
    for c in copies_y + copies_x:
        c.wait_send()


def combine(dims, basis, small, corr_hbm, new_hbm, est_ref, corr, new, sems):
    nf, cx, cy, nz = dims
    nt = nz // LANES
    nb = (DEPTH + 1) * nf
    weights = small[0:2 * nf, 0:nb]
    copies = []
    for x in range(cx):
        at = x * cy * nz
        part = basis[:, at:at + cy * nz]
        out = lax.dot_general(weights, part, (((1,), (0,)), ((), ())), precision=lax.Precision.HIGHEST,
                              preferred_element_type=jnp.float32)
        for y in range(cy):
            for t in range(nt):
                span = slice(y * nz + t * LANES, y * nz + (t + 1) * LANES)
                rows = pl.ds(t * cy + y, nf, stride=nt * cy)
                corr[x, rows, :] = out[0:nf, span]
                new[x, rows, :] = part[0:nf, span] - out[nf:2 * nf, span]
        for i, (src, dst) in enumerate(((corr, corr_hbm), (new, new_hbm))):
            for f in range(nf):
                c = pltpu.make_async_copy(src.at[x, pl.ds(f * nt * cy, nt * cy)],
                                          dst.at[pl.ds((f * cx + x) * nt * cy, nt * cy)], sems.at[i, x, f])
                c.start()
                copies.append(c)
    est_ref[...] = small[2 * nf:2 * nf + 1, 0:nf]
    for c in copies:
        c.wait()


def solution(mesh):
    nx, ny = mesh.shape["gx"], mesh.shape["gy"]

    def body(residual_block, diagonal):
        nf, cx, cy, nz = residual_block.shape
        nb = (DEPTH + 1) * nf
        wx, wy = cx + 2 * DEPTH, cy + 2 * DEPTH
        nt = nz // LANES
        flat = jax.ShapeDtypeStruct((nf * cx * nt * cy, LANES), jnp.float32)

        def tiles(v):
            return v.reshape(nf, cx, cy, nt, LANES).transpose(0, 1, 3, 2, 4).reshape(flat.shape)

        def untile(v):
            return v.reshape(nf, cx, nt, cy, LANES).transpose(0, 1, 3, 2, 4).reshape(nf, cx, cy, nz)

        assert cx == DEPTH and nx % 2 == 0
        halo_slots = 2 * (DEPTH + 1) + 4 + 4 * (DEPTH + 1)
        vmem = pl.BlockSpec(memory_space=pltpu.VMEM)
        hbm = pl.BlockSpec(memory_space=pltpu.HBM)
        basis, small = pl.pallas_call(
            functools.partial(kernel, nx, ny, (nf, cx, cy, nz)),
            out_shape=(jax.ShapeDtypeStruct((nb, cx * cy * nz), jnp.float32),
                       jax.ShapeDtypeStruct((3 * nf, LANES), jnp.float32)),
            in_specs=[hbm, hbm],
            out_specs=(vmem, vmem),
            scratch_shapes=[
                pltpu.VMEM(flat.shape, jnp.float32),
                pltpu.VMEM(diagonal.shape, jnp.float32),
                pltpu.SemaphoreType.DMA((2,)),
                pltpu.VMEM((DEPTH, wx, wy, nf, nz), jnp.float32),
                pltpu.VMEM((DEPTH, wx, wy, nf, nz), jnp.float32),
                pltpu.VMEM((wx, 3, cy, nz), jnp.float32),
                pltpu.VMEM((nb, LANES), jnp.float32),
                pltpu.VMEM((ny, nf, LANES), jnp.float32),
                pltpu.VMEM((nx, nf, LANES), jnp.float32),
                pltpu.VMEM((LANES, LANES), jnp.float32),
                pltpu.SemaphoreType.DMA((halo_slots,)),
                pltpu.SemaphoreType.DMA((halo_slots,)),
                pltpu.SemaphoreType.DMA((ny,)),
                pltpu.SemaphoreType.DMA((ny,)),
                pltpu.SemaphoreType.DMA((nx,)),
                pltpu.SemaphoreType.DMA((nx,)),
            ],
            compiler_params=pltpu.CompilerParams(collective_id=0, has_side_effects=True, vmem_limit_bytes=24 << 20),
        )(pltpu.with_memory_space_constraint(tiles(residual_block), pltpu.HBM),
          pltpu.with_memory_space_constraint(diagonal, pltpu.HBM))
        corr, new, est = pl.pallas_call(
            functools.partial(combine, (nf, cx, cy, nz)),
            out_shape=(flat, flat, jax.ShapeDtypeStruct((1, nf), jnp.float32)),
            in_specs=[vmem, vmem],
            out_specs=(hbm, hbm, vmem),
            scratch_shapes=[
                pltpu.VMEM((cx, nf * nt * cy, LANES), jnp.float32),
                pltpu.VMEM((cx, nf * nt * cy, LANES), jnp.float32),
                pltpu.SemaphoreType.DMA((2, cx, nf)),
            ],
            compiler_params=pltpu.CompilerParams(vmem_limit_bytes=8 << 20),
        )(basis, small)
        return untile(corr), untile(new), est.reshape(nf)

    return jax.shard_map(body, mesh=mesh, in_specs=(P(None, "gx", "gy", None), P("gx", "gy", None)),
                         out_specs=(P(None, "gx", "gy", None), P(None, "gx", "gy", None), P()), check_vma=False)
```

```python
import functools

import jax
import jax.numpy as jnp
from jax import lax
from jax.experimental import pallas as pl
from jax.experimental.pallas import tpu as pltpu
from jax.sharding import PartitionSpec as P

WEIGHT_X = 0.4
WEIGHT_Y = 0.2
WEIGHT_Z = 0.1
CENTRE = 2.2
SCALE_POWER = 3.0
SHIFTS = (6.0, 1.5, 4.5, 3.0)
EPSILON = 1e-06
DEPTH = len(SHIFTS)
MESH = pl.DeviceIdType.MESH
LANES = 128


def kernel(nx, ny, dims, r_hbm, d_hbm, basis, small_ref, r_ref, d_ref, load_sem,
           e_bufs, sy, dd, gram, gather_y, gather_x, wide, halo_send, halo_recv, red_send_y, red_recv_y,
           red_send_x, red_recv_x, known):
    nf, cx, cy, nz = dims
    dep = DEPTH
    nb = (dep + 1) * nf
    nk = dep * nf
    gx = lax.axis_index("gx")
    gy = lax.axis_index("gy")
    e0 = e_bufs.at[0]
    wx, wy = cx + 2 * dep, cy + 2 * dep
    nt = nz // LANES

    even = lax.rem(gx, 2) == 0
    partner = jnp.where(even, gx + 1, gx - 1)
    beyond = jnp.where(even, gx + 2, gx - 2)
    has_up, has_down = gx < nx - 2, gx >= 2
    gx_peers = 1 + jnp.where(has_up, 1, 0) + jnp.where(has_down, 1, 0)

    def greet(sem):
        pl.semaphore_signal(sem, inc=1, device_id=(partner, gy), device_id_type=MESH)
        pl.when(has_up)(lambda: pl.semaphore_signal(sem, inc=1, device_id=(gx + 2, gy), device_id_type=MESH))
        pl.when(has_down)(lambda: pl.semaphore_signal(sem, inc=1, device_id=(gx - 2, gy), device_id_type=MESH))

    barrier = pltpu.get_barrier_semaphore()
    greet(barrier)
    for k in range(1, ny):
        pl.semaphore_signal(barrier, inc=1, device_id=(gx, lax.rem(gy + k, ny)), device_id_type=MESH)
    rounds = nx // 2 - 1
    done = []

    def next_round():
        if len(done) < rounds:
            pl.semaphore_wait(known.at[len(done)], gx_peers)
            done.append(1)
            if len(done) < rounds:
                greet(known.at[len(done)])

    loads = [pltpu.make_async_copy(r_hbm, r_ref, load_sem.at[0]), pltpu.make_async_copy(d_hbm, d_ref, load_sem.at[1])]
    for c in loads:
        c.start()
    can_forward = (beyond >= 0) & (beyond < nx)
    gets_forward = (gx > 0) & (gx < nx - 1)
    has_right, has_left = gy < ny - 1, gy > 0
    near = jnp.where(even, dep + cx, 0)
    far = jnp.where(even, 0, dep + cx)

    @pl.when(jnp.logical_not(gets_forward))
    def _():
        def one(i, c):
            e0[far + i] = jnp.zeros((wy, nf, nz), jnp.float32)
            dd[far + i] = jnp.zeros((3, cy, nz), jnp.float32)
            return c
        lax.fori_loop(0, dep, one, 0)

    def clear_cols(lo, tile):
        def one(i, c):
            e0[i, lo:lo + dep] = jnp.zeros((dep, nf, nz), jnp.float32)
            dd[i, tile] = jnp.zeros((cy, nz), jnp.float32)
            return c
        lax.fori_loop(0, wx, one, 0)

    pl.when(gy == 0)(lambda: clear_cols(0, 0))
    pl.when(gy == ny - 1)(lambda: clear_cols(dep + cy, 2))

    for c in loads:
        c.wait()

    for x in range(cx):
        for y in range(cy):
            v = jnp.concatenate([r_ref[pl.ds((x * nt + t) * cy + y, nf, stride=cx * cy * nt), :] for t in range(nt)], 1)
            e0[dep + x, dep + y] = v
            cell = x * cy + y
            basis[0:nf, cell * nz:(cell + 1) * nz] = v
        dd[dep + x, 1] = d_ref[x]

    pl.semaphore_wait(barrier, gx_peers + ny - 1)
    if rounds > 0:
        greet(known.at[0])

    def copy(src, dst, slot, dev):
        return pltpu.make_async_remote_copy(src_ref=src, dst_ref=dst, send_sem=halo_send.at[slot],
                                            recv_sem=halo_recv.at[slot], device_id=dev, device_id_type=MESH)

    pieces = [(i, h) for i in range(cx) for h in range(2)]
    pieces.insert(2, None)
    count = len(pieces)
    left_half, right_half = pl.ds(dep, dep), pl.ds(cy, dep)

    def block(src, dev, slot):
        out = []
        for k, piece in enumerate(pieces):
            if piece is None:
                out.append(copy(dd.at[pl.ds(src, cx), 1], dd.at[pl.ds(far, cx), 1], slot + k, dev))
            else:
                half = (left_half, right_half)[piece[1]]
                out.append(copy(e0.at[src + piece[0], half], e0.at[far + piece[0], half], slot + k, dev))
        return out

    swap = block(dep, (partner, gy), 0)
    forward = block(near, (beyond, gy), count)
    right, left = (gx, gy + 1), (gx, gy - 1)

    def d_edges(rows, slot):
        return (copy(dd.at[rows, 1], dd.at[rows, 0], slot, right), copy(dd.at[rows, 1], dd.at[rows, 2], slot + 1, left))

    def e_edges(rows, slot):
        return (copy(e0.at[rows, right_half], e0.at[rows, pl.ds(0, dep)], slot, right),
                copy(e0.at[rows, left_half], e0.at[rows, pl.ds(dep + cy, dep)], slot + 1, left))

    def block_edges(src, slot):
        out = []
        for k, piece in enumerate(pieces):
            if piece is None:
                out.append(d_edges(pl.ds(src, cx), slot + 2 * k))
            else:
                pair = e_edges(src + piece[0], slot + 2 * k)
                out.append((None, pair[1]) if piece[1] == 0 else (pair[0], None))
        return out

    base = 2 * count
    own_edges = [d_edges(pl.ds(dep, cx), base), e_edges(pl.ds(dep, cx), base + 2)]
    near_edges = block_edges(near, base + 4)
    far_edges = block_edges(far, base + 4 + 2 * count)

    def when(pred, act):
        pl.when(pred)(act)

    def each(pred, pairs, act, other=False):
        for side, has in ((0, has_left if other else has_right), (1, has_right if other else has_left)):
            def go(side=side):
                for pair in pairs:
                    if pair[side] is not None:
                        act(pair[side])
            if any(pair[side] is not None for pair in pairs):
                when(has & pred, go)

    def start_edges(pairs, pred=True):
        each(pred, pairs, lambda c: c.start())

    def wait_edges(pairs, pred=True):
        each(pred, pairs, lambda c: c.wait_recv(), other=True)

    for c in swap:
        c.start()
    start_edges(own_edges)
    for i in range(count):
        swap[i].wait_recv()
        when(can_forward, lambda i=i: forward[i].start())
        start_edges(near_edges[i:i + 1])
    next_round()

    def take_far(lo, hi):
        for i in range(lo, min(hi, count)):
            when(gets_forward, lambda i=i: forward[i].wait_recv())
            start_edges(far_edges[i:i + 1], gets_forward)

    lane = lax.broadcasted_iota(jnp.int32, (nf, nz), 1)
    first, last = lane == 0, lane == nz - 1

    def sum_z(v):
        lo = jnp.where(first, 0.0, pltpu.roll(v, 1, 1))
        hi = jnp.where(last, 0.0, pltpu.roll(v, nz - 1, 1))
        return v + WEIGHT_Z * (lo + hi)

    total_x, total_y = cx * nx, cy * ny

    def row_pass(j, x):
        src = e_bufs.at[j]
        prev = sum_z(src[x, j])
        here = sum_z(src[x, j + 1])
        for y in range(j + 1, wy - j - 1):
            nxt = sum_z(src[x, y + 1])
            sy[j, x, y] = here + WEIGHT_Y * (prev + nxt)
            prev, here = here, nxt

    def col_pass(j, x):
        at_x = gx * cx + x - dep
        in_x = (at_x >= 0) & (at_x < total_x)
        for y in range(j + 1, wy - j - 1):
            at_y = gy * cy + y - dep
            factor = jnp.where(in_x & (at_y >= 0) & (at_y < total_y), 1.0 / SCALE_POWER, 0.0)
            tile, sub = (y - dep + cy) // cy, (y - dep) % cy
            diag = dd[x, tile, sub:sub + 1, :]
            s = sy[j, x, y] + WEIGHT_X * (sy[j, x - 1, y] + sy[j, x + 1, y])
            v = ((CENTRE + 1.0 - SHIFTS[j] + diag) * e_bufs[j, x, y] - s) * factor
            if j + 1 < dep:
                e_bufs[j + 1, x, y] = v
            else:
                cell = (x - dep) * cy + (y - dep)
                basis[dep * nf:(dep + 1) * nf, pl.ds(pl.multiple_of(cell * nz, nz), nz)] = v

    def sweep(one, j, lo, count):
        def body(i, c):
            one(j, lo + i)
            return c
        if count > 0:
            lax.fori_loop(0, count, body, 0)

    take_far(0, 5)
    wait_edges(own_edges)
    wait_edges(near_edges)
    take_far(5, 7)
    for j in range(dep):
        lo = jnp.where(even, dep + j, j)
        sweep(row_pass, j, lo, cx + dep - 2 * j)
        sweep(col_pass, j, lo + 1, cx + dep - 2 - 2 * j)
        if j == 0:
            take_far(7, count)
            next_round()
    wait_edges(far_edges, gets_forward)
    for j in range(dep):
        sweep(row_pass, j, jnp.where(even, j, cx + dep - j), dep)
        sweep(col_pass, j, jnp.where(even, j + 1, cx + dep - 1 - j), dep)
    for j in range(1, dep):
        for cell in range(cx * cy):
            basis[j * nf:(j + 1) * nf, cell * nz:(cell + 1) * nz] = e_bufs[j, dep + cell // cy, dep + cell % cy]

    b = basis[...]
    local = lax.dot_general(b, b, (((1,), (1,)), ((), ())), precision=lax.Precision.HIGHEST,
                            preferred_element_type=jnp.float32)
    gram[...] = jnp.zeros_like(gram)
    gram[:, 0:nb] = local

    def reduce(buf, value, me, n, send, recv, dev):
        buf[me] = value
        copies = []
        for k in range(1, n):
            to = lax.rem(me + k, n)
            c = pltpu.make_async_remote_copy(src_ref=buf.at[me], dst_ref=buf.at[me], send_sem=send.at[k],
                                             recv_sem=recv.at[k], device_id=dev(to), device_id_type=MESH)
            c.start()
            copies.append(c)
        for k in range(1, n):
            frm = lax.rem(me - k + n, n)
            pltpu.make_async_remote_copy(src_ref=buf.at[frm], dst_ref=buf.at[frm], send_sem=send.at[k],
                                         recv_sem=recv.at[k], device_id=dev(frm), device_id_type=MESH).wait_recv()
        total = buf[0]
        for k in range(1, n):
            total = total + buf[k]
        return total, copies

    lane_f = lax.broadcasted_iota(jnp.int32, (nf, LANES), 1)

    def turn(v, by):
        return pltpu.roll(v, by % LANES, 1) if by % LANES else v

    packed = jnp.zeros((nf, LANES), jnp.float32)
    for j in range(dep + 1):
        kept = jnp.where(lane_f < (j + 1) * nf, gram[j * nf:(j + 1) * nf, :], 0.0)
        packed = packed + turn(kept, nf * j * (j + 1) // 2)
    part, copies_y = reduce(gather_y, packed, gy, ny, red_send_y, red_recv_y, lambda t: (gx, t))
    for _ in range(rounds):
        next_round()
    whole, copies_x = reduce(gather_x, part, gx, nx, red_send_x, red_recv_x, lambda t: (t, gy))
    wide[...] = jnp.zeros_like(wide)
    for j in range(dep + 1):
        wide[j * nf:(j + 1) * nf, :] = jnp.where(lane_f < (j + 1) * nf, turn(whole, -(nf * j * (j + 1) // 2)), 0.0)
    lower = wide[...]
    upper = jnp.transpose(lower)[0:nb]
    lower = lower[0:nb]
    block_row = lax.broadcasted_iota(jnp.int32, (nb, LANES), 0) // nf
    full = jnp.where(lax.broadcasted_iota(jnp.int32, (nb, LANES), 1) < (block_row + 1) * nf, lower, upper)

    lane_b = lax.broadcasted_iota(jnp.int32, (nb, LANES), 1)
    sigma_lane = jnp.zeros((nb, LANES), jnp.float32)
    for j, shift in enumerate(SHIFTS):
        sigma_lane = jnp.where((lane_b >= j * nf) & (lane_b < (j + 1) * nf), shift, sigma_lane)
    gn = full * sigma_lane + SCALE_POWER * pltpu.roll(full, LANES - nf, 1)

    def newton_rows(m):
        return jnp.concatenate([SHIFTS[j] * m[j * nf:(j + 1) * nf] + SCALE_POWER * m[(j + 1) * nf:(j + 2) * nf]
                                for j in range(dep)], 0)

    image = newton_rows(gn)
    right_side = pltpu.roll(newton_rows(full), nk, 1)
    lane_k = lax.broadcasted_iota(jnp.int32, (nk, LANES), 1)
    row_k = lax.broadcasted_iota(jnp.int32, (nk, LANES), 0)
    on_diag = jnp.where(lane_k == row_k, image, 0.0)
    s_col = lax.rsqrt(jnp.sum(on_diag, axis=1, keepdims=True) + EPSILON)
    s_row = lax.rsqrt(jnp.sum(on_diag, axis=0, keepdims=True) + EPSILON)
    in_image = lane_k < nk
    in_right = (lane_k >= nk) & (lane_k < nk + nf)
    m = jnp.where(in_image, image * s_col * s_row, jnp.where(in_right, right_side * s_col, 0.0))
    for k in range(nk):
        row = m[k:k + 1, :]
        row = row / row[:, k:k + 1]
        m = jnp.where(row_k == k, row, m - m[:, k:k + 1] * row)
    coeffs = jnp.where(in_right, m * s_col, 0.0)

    diag0 = jnp.sum(jnp.where(lane_k[:nf] == row_k[:nf], full[:nf], 0.0), axis=0, keepdims=True)
    used = pltpu.roll(jnp.sum(jnp.where(in_right, right_side * coeffs, 0.0), axis=0, keepdims=True), LANES - nk, 1)
    blocks = [coeffs[j * nf:(j + 1) * nf] for j in range(dep)]
    combined = [SHIFTS[0] * blocks[0]]
    for j in range(1, dep):
        combined.append(SHIFTS[j] * blocks[j] + SCALE_POWER * blocks[j - 1])
    combined.append(SCALE_POWER * blocks[dep - 1])
    wide[...] = jnp.zeros_like(wide)
    for j in range(dep + 1):
        moved = pltpu.roll(combined[j], nf, 1)
        wide[j * nf:(j + 1) * nf, :] = moved + blocks[j] if j < dep else moved
    small_ref[0:2 * nf, :] = jnp.transpose(wide[...])[nk:nk + 2 * nf, :]
    small_ref[2 * nf:, :] = jnp.broadcast_to((diag0 - used) / jnp.where(lane_k[:1] < nf, diag0, 1.0), (nf, LANES))

    for i in range(count):
        swap[i].wait_send()

    @pl.when(can_forward)
    def _():
        for i in range(count):
            forward[i].wait_send()

    for pairs, pred in ((own_edges, True), (near_edges, True), (far_edges, gets_forward)):
        each(pred, pairs, lambda c: c.wait_send())
    for c in copies_y + copies_x:
        c.wait_send()


def combine(dims, basis, small, corr_hbm, new_hbm, est_ref, corr, new, sems):
    nf, cx, cy, nz = dims
    nt = nz // LANES
    nb = (DEPTH + 1) * nf
    weights = small[0:2 * nf, 0:nb]
    copies = []
    for x in range(cx):
        at = x * cy * nz
        part = basis[:, at:at + cy * nz]
        out = lax.dot_general(weights, part, (((1,), (0,)), ((), ())), precision=lax.Precision.HIGHEST,
                              preferred_element_type=jnp.float32)
        for y in range(cy):
            for t in range(nt):
                span = slice(y * nz + t * LANES, y * nz + (t + 1) * LANES)
                rows = pl.ds(t * cy + y, nf, stride=nt * cy)
                corr[x, rows, :] = out[0:nf, span]
                new[x, rows, :] = part[0:nf, span] - out[nf:2 * nf, span]
        for i, (src, dst) in enumerate(((corr, corr_hbm), (new, new_hbm))):
            for f in range(nf):
                c = pltpu.make_async_copy(src.at[x, pl.ds(f * nt * cy, nt * cy)],
                                          dst.at[pl.ds((f * cx + x) * nt * cy, nt * cy)], sems.at[i, x, f])
                c.start()
                copies.append(c)
    est_ref[...] = small[2 * nf:2 * nf + 1, 0:nf]
    for c in copies:
        c.wait()


def solution(mesh):
    nx, ny = mesh.shape["gx"], mesh.shape["gy"]

    def body(residual_block, diagonal):
        nf, cx, cy, nz = residual_block.shape
        nb = (DEPTH + 1) * nf
        wx, wy = cx + 2 * DEPTH, cy + 2 * DEPTH
        nt = nz // LANES
        flat = jax.ShapeDtypeStruct((nf * cx * nt * cy, LANES), jnp.float32)

        def tiles(v):
            return v.reshape(nf, cx, cy, nt, LANES).transpose(0, 1, 3, 2, 4).reshape(flat.shape)

        def untile(v):
            return v.reshape(nf, cx, nt, cy, LANES).transpose(0, 1, 3, 2, 4).reshape(nf, cx, cy, nz)

        assert cx == DEPTH and cy == 2 * DEPTH and nx % 2 == 0
        halo_slots = 6 * (2 * cx + 1) + 4
        vmem = pl.BlockSpec(memory_space=pltpu.VMEM)
        hbm = pl.BlockSpec(memory_space=pltpu.HBM)
        basis, small = pl.pallas_call(
            functools.partial(kernel, nx, ny, (nf, cx, cy, nz)),
            out_shape=(jax.ShapeDtypeStruct((nb, cx * cy * nz), jnp.float32),
                       jax.ShapeDtypeStruct((3 * nf, LANES), jnp.float32)),
            in_specs=[hbm, hbm],
            out_specs=(vmem, vmem),
            scratch_shapes=[
                pltpu.VMEM(flat.shape, jnp.float32),
                pltpu.VMEM(diagonal.shape, jnp.float32),
                pltpu.SemaphoreType.DMA((2,)),
                pltpu.VMEM((DEPTH, wx, wy, nf, nz), jnp.float32),
                pltpu.VMEM((DEPTH, wx, wy, nf, nz), jnp.float32),
                pltpu.VMEM((wx, 3, cy, nz), jnp.float32),
                pltpu.VMEM((nb, LANES), jnp.float32),
                pltpu.VMEM((ny, nf, LANES), jnp.float32),
                pltpu.VMEM((nx, nf, LANES), jnp.float32),
                pltpu.VMEM((LANES, LANES), jnp.float32),
                pltpu.SemaphoreType.DMA((halo_slots,)),
                pltpu.SemaphoreType.DMA((halo_slots,)),
                pltpu.SemaphoreType.DMA((ny,)),
                pltpu.SemaphoreType.DMA((ny,)),
                pltpu.SemaphoreType.DMA((nx,)),
                pltpu.SemaphoreType.DMA((nx,)),
                pltpu.SemaphoreType.REGULAR((max(nx // 2 - 1, 1),)),
            ],
            compiler_params=pltpu.CompilerParams(collective_id=0, has_side_effects=True, vmem_limit_bytes=24 << 20),
        )(pltpu.with_memory_space_constraint(tiles(residual_block), pltpu.HBM),
          pltpu.with_memory_space_constraint(diagonal, pltpu.HBM))
        corr, new, est = pl.pallas_call(
            functools.partial(combine, (nf, cx, cy, nz)),
            out_shape=(flat, flat, jax.ShapeDtypeStruct((1, nf), jnp.float32)),
            in_specs=[vmem, vmem],
            out_specs=(hbm, hbm, vmem),
            scratch_shapes=[
                pltpu.VMEM((cx, nf * nt * cy, LANES), jnp.float32),
                pltpu.VMEM((cx, nf * nt * cy, LANES), jnp.float32),
                pltpu.SemaphoreType.DMA((2, cx, nf)),
            ],
            compiler_params=pltpu.CompilerParams(vmem_limit_bytes=8 << 20),
        )(basis, small)
        return untile(corr), untile(new), est.reshape(nf)

    return jax.shard_map(body, mesh=mesh, in_specs=(P(None, "gx", "gy", None), P("gx", "gy", None)),
                         out_specs=(P(None, "gx", "gy", None), P(None, "gx", "gy", None), P()), check_vma=False)
```
